32 devices in a mesh: expert: 8 (over z, y), dp: 4 (over x, core).
Axes of the slice: x: 2, y: 2, z: 4, core: 2. Of those that a mesh axis runs over, the one named last changes fastest.
Arguments:
- tokens: bfloat16 [2048, 2880], P(('expert', 'dp')), may hold values from -6 to 6
- expert_ids: int32 [2048, 4], P(('expert', 'dp')), may hold values from 0 to 7, all different within a row; in each aligned block of 64 rows (0 to 63, 64 to 127, ...) at most 48 rows name the same one
- gate_logits: float32 [2048, 4], P(('expert', 'dp')), may hold values from -3 to 3
- w_gate: bfloat16 [8, 2880, 1536], P('expert', None, 'dp'), may hold values from -0.109375 to 0.109375
- w_up: bfloat16 [8, 2880, 1536], P('expert', None, 'dp'), may hold values from -0.109375 to 0.109375
- w_down: bfloat16 [8, 1536, 2880], P('expert', 'dp'), may hold values from -0.15625 to 0.15625
Outputs:
- mixed: bfloat16 [2048, 2880], P(('expert', 'dp'))
The draws below stay inside these ranges and needn't reach their ends.
Inputs may be any that keep to these rules, and one draw needn't show every extreme that they name: `expert_ids`: each row names 4 different experts. Among the 64 rows of one device no expert is named more than 48 times, and every expert is named somewhere.
All inputs are finite; a program needn't handle non-finite values.
Results may differ from the reference program's by a relative error of at most 0.012.
Values may be sent and summed in bfloat16 or wider, within the bound.
A program may use at most 128 MiB of HBM per device.

```python
import math
import jax
import jax.numpy as jnp
import numpy as np
from jax import lax

D = 2880
FF = 1536
TOP = 4
TOK_DEV = 64
EXPERTS = 8
CAP = 48
TOKENS = 2048
N_EXPERT = 8
N_DP = 4


def levels(rng, dims, split, smallest, largest):
    loudness, own = 1.0, jax.random.fold_in(rng, 6)
    for dim, shards_of in split:
        steps = jnp.exp(jax.random.uniform(jax.random.fold_in(own, dim), (shards_of,), jnp.float32, smallest / len(split), largest / len(split)))
        loudness = loudness * jnp.repeat(steps, dims[dim] // shards_of).reshape([-1 if axis == dim else 1 for axis in range(len(dims))])
    return loudness


def shared_out(key, own, number, rows, count, top, most, lean):
    order = jax.random.permutation(key, count)
    crowded, common = shares(count, rows * top, most, lean, True), shares(count, rows * top, most, lean, False)
    places = jnp.arange(count)

    def named(tallies, rotation):
        used = int((tallies > 0).sum())
        fixed = max(1, used // 4)
        moved = fixed + (places - fixed + rotation * (used - fixed)) % max(1, count - fixed)
        return jnp.zeros((count,), jnp.int32).at[order[jnp.where(places < fixed, places, moved)]].set(jnp.asarray(tallies, jnp.int32))

    tallies = jnp.where(number % 4 == 0, named(crowded, number // 4), named(common, number - number // 4 - 1))
    mixed = jax.random.permutation(jax.random.fold_in(own, 3), count)
    source_of, taker = mixed[0:count // 2 * 2:2], mixed[1:count // 2 * 2:2]
    room = jnp.minimum(tallies[source_of] - 1, most - tallies[taker]) // 2
    room = jnp.where((source_of == order[0]) | (taker == order[0]) | (tallies[taker] == 0), 0, jnp.maximum(room, 0))
    moved = jax.random.randint(jax.random.fold_in(own, 4), (count // 2,), 0, 1 << 20) % (room + 1)
    tallies = tallies.at[source_of].add(-moved).at[taker].add(moved)
    labels = jnp.searchsorted(jnp.cumsum(tallies), jnp.arange(rows * top), side="right").astype(jnp.int32)
    table = labels.reshape(top, rows).T
    table = table[jax.random.permutation(jax.random.fold_in(own, 1), rows)]
    rotation = jax.random.randint(jax.random.fold_in(own, 2), (rows, 1), 0, top)
    return jnp.take_along_axis(table, (jnp.arange(top)[None, :] + rotation) % top, axis=1)


def shares(amount, total, limit, skew, full):
    weights = [(1 << 20) // math.isqrt(standing ** skew) + 1 for standing in range(1, amount + 1)]
    largest = limit if full else min(limit, max(-(-total // amount), total * weights[0] // sum(weights)))
    least = 1 if total - largest >= amount - 1 else 0
    given, spare = [largest] + [least] * (amount - 1), total - largest - least * (amount - 1)
    while spare > 0:
        movable = [i for i in range(1, amount) if given[i] < largest] or [i for i in range(1, amount) if given[i] < limit]
        mass, left = sum([weights[i] for i in movable]), spare
        for i in movable:
            addition = min(limit - given[i], max(1, left * weights[i] // mass), spare)
            given[i] = given[i] + addition
            spare = spare - addition
    return np.array(given)


def normal_values(key, extent, scale, most, split=(), kind=jnp.bfloat16):
    result = jax.random.normal(key, extent, jnp.float32) * scale
    if len(split) > 0:
        result = levels(key, extent, split, -0.22, 0.18) * result
    return jnp.clip(result, min=-most, max=most).astype(kind)


def setup_inputs(seed: int = 0) -> dict:
    key_list = jax.random.split(jax.random.key(seed), 7)
    tokens = normal_values(key_list[0], (TOKENS, D), 1.0, 6.0, ((0, 32),))
    expert_ids_keys = jax.random.split(jax.random.fold_in(key_list[1], 1), TOKENS // TOK_DEV)
    expert_ids_turns = jax.random.permutation(jax.random.fold_in(key_list[1], 3), TOKENS // TOK_DEV)
    expert_ids = jax.vmap(lambda own, number: shared_out(jax.random.fold_in(key_list[1], 2), own, number, TOK_DEV, EXPERTS, TOP, CAP, 2))(expert_ids_keys, expert_ids_turns).reshape((TOKENS, TOP))
    gate_logits = jnp.clip(jax.random.uniform(key_list[2], (TOKENS, TOP), jnp.float32, -3.0, 3.0) * levels(key_list[2], (TOKENS, TOP), ((0, 32),), -0.4, 0.0), -3.0, 3.0)
    w_gate = normal_values(key_list[3], (EXPERTS, D, FF), D ** -0.5, 0.109375, ((0, 8), (2, 4)))
    w_up = normal_values(key_list[4], (EXPERTS, D, FF), D ** -0.5, 0.109375, ((0, 8), (2, 4)))
    w_down = normal_values(key_list[5], (EXPERTS, FF, D), FF ** -0.5, 0.15625, ((0, 8), (1, 4)))
    return dict(tokens=tokens, expert_ids=expert_ids, gate_logits=gate_logits, w_gate=w_gate, w_up=w_up, w_down=w_down)


def expert_rows(rows_in, gate_w, up_w, down_w):
    quarter = gate_w.shape[1] // N_DP
    summed = jnp.zeros((rows_in.shape[0], down_w.shape[1]), jnp.float32)
    for index_q in range(N_DP):
        low_col = index_q * quarter
        high_col = low_col + quarter
        gate_val = jnp.dot(rows_in, gate_w[:, low_col:high_col], preferred_element_type=jnp.float32)
        up_val = jnp.dot(rows_in, up_w[:, low_col:high_col], preferred_element_type=jnp.float32)
        hidden = ((up_val + 1.0) * gate_val * jax.nn.sigmoid(1.702 * gate_val)).astype(jnp.bfloat16)
        partial_value = jnp.dot(hidden, down_w[low_col:high_col], preferred_element_type=jnp.float32).astype(jnp.bfloat16)
        summed = summed + lax.optimization_barrier(partial_value).astype(jnp.float32)
    return summed.astype(jnp.bfloat16)


def reference(tokens, expert_ids, gate_logits, w_gate, w_up, w_down):
    n_assign = TOKENS * TOP
    flat_ids = expert_ids.reshape(-1).astype(jnp.int32)
    sorter = jnp.argsort(flat_ids, stable=True).astype(jnp.int32)
    counts = jnp.sum((flat_ids[:, None] == jnp.arange(EXPERTS, dtype=jnp.int32)[None, :]).astype(jnp.int32), axis=0)
    starts = (jnp.cumsum(counts) - counts).astype(jnp.int32)
    longest = N_EXPERT * N_DP * CAP
    padded_order = jnp.concatenate([sorter, jnp.zeros((longest,), jnp.int32)])

    def per_expert(expert):
        chosen = lax.dynamic_slice_in_dim(padded_order, starts[expert], longest)
        rows_in = tokens[chosen // TOP]
        return expert_rows(rows_in, w_gate[expert], w_up[expert], w_down[expert])

    outputs_all = lax.map(per_expert, jnp.arange(EXPERTS, dtype=jnp.int32))
    inverse = jnp.zeros((n_assign,), jnp.int32).at[sorter].set(jnp.arange(n_assign, dtype=jnp.int32))
    rank_in = (inverse - starts[flat_ids]).astype(jnp.int32)
    picked = outputs_all.reshape(-1, D)[flat_ids * longest + rank_in]
    gate_wts = jnp.exp(gate_logits.astype(jnp.float32))
    gate_wts = gate_wts / jnp.sum(gate_wts, axis=1, keepdims=True)
    mixed = jnp.sum(picked.reshape(TOKENS, TOP, D).astype(jnp.float32) * gate_wts[:, :, None], axis=1)
    return mixed.astype(jnp.bfloat16)
```

```python
import functools

import jax
import jax.numpy as jnp
from jax import lax
from jax.experimental import pallas as pl
from jax.experimental.pallas import tpu as pltpu
from jax.sharding import PartitionSpec as P


def expert_rows(tile_in, gate_w, up_w, down_w):
    gate_val = jnp.dot(tile_in, gate_w, preferred_element_type=jnp.float32)
    up_val = jnp.dot(tile_in, up_w, preferred_element_type=jnp.float32)
    hidden = ((up_val + 1.0) * gate_val * jax.nn.sigmoid(1.702 * gate_val)).astype(jnp.bfloat16)
    return jnp.dot(hidden, down_w, preferred_element_type=jnp.float32).astype(jnp.bfloat16)


def run_tiles(packed, first_row, last_row, gate_w, up_w, down_w):
    tile_rows = 128
    n_tiles = jnp.maximum(last_row - first_row + tile_rows - 1, 0) // tile_rows
    result_buf = jnp.zeros((packed.shape[0], down_w.shape[1]), jnp.bfloat16)

    def advance(index_t, buffer):
        at_row = first_row + index_t * tile_rows
        tile_in = lax.dynamic_slice_in_dim(packed, at_row, tile_rows, 0)
        return lax.dynamic_update_slice_in_dim(
            buffer, expert_rows(tile_in, gate_w, up_w, down_w), at_row, 0
        )

    return lax.fori_loop(0, n_tiles, advance, result_buf)


def sparse_device(tokens, expert_ids, gate_logits, w_gate, w_up, w_down):
    n_rows, width = tokens.shape
    n_tops = expert_ids.shape[1]
    n_exp = lax.axis_size("expert")
    n_dp = lax.axis_size("dp")
    slot_cap = max(2, 3 * n_rows * n_tops // (2 * n_exp))
    tile_rows = 128
    flat_ids = expert_ids.reshape(-1)
    onehot = (flat_ids[:, None] == jnp.arange(n_exp, dtype=jnp.int32)[None, :]).astype(jnp.int32)
    rank_in = jnp.sum((jnp.cumsum(onehot, axis=0) - onehot) * onehot, axis=1)
    counts = jnp.sum(onehot, axis=0)
    slot_idx = flat_ids * slot_cap + rank_in
    source = (
        jnp.zeros((n_exp * slot_cap,), jnp.int32)
        .at[slot_idx]
        .set(jnp.arange(n_rows * n_tops, dtype=jnp.int32) // n_tops)
    )
    filled = (jnp.arange(slot_cap)[None, :] < counts[:, None]).reshape(-1)
    outgoing = jnp.where(filled[:, None], tokens[source], jnp.zeros_like(tokens[source])).reshape(
        n_exp, slot_cap, width
    )
    rows_mid, counts_mid = (
        lax.all_to_all(outgoing, "expert", split_axis=0, concat_axis=0, tiled=True),
        lax.all_to_all(counts[:, None], "expert", split_axis=0, concat_axis=0, tiled=True),
    )
    rows_in, counts_in = (
        lax.all_gather(rows_mid, "dp", axis=0, tiled=True),
        lax.all_gather(counts_mid, "dp", axis=0, tiled=True),
    )
    rows_flat = rows_in.reshape(-1, width)
    total_rows = rows_flat.shape[0]
    live_row = (jnp.arange(slot_cap)[None, :] < counts_in.reshape(-1)[:, None]).reshape(-1)
    position = jnp.cumsum(live_row.astype(jnp.int32)) - 1
    live_total = jnp.sum(live_row.astype(jnp.int32))
    padded = (total_rows + tile_rows - 1) // tile_rows * tile_rows + tile_rows
    gather_idx = (
        jnp.zeros((padded,), jnp.int32)
        .at[jnp.where(live_row, position, padded)]
        .set(jnp.arange(total_rows, dtype=jnp.int32), mode="drop")
    )
    packed = rows_flat[gather_idx]
    gate_w = w_gate[0]
    up_w = w_up[0]
    down_w = w_down[0]
    merged = run_tiles(packed, 0, live_total, gate_w, up_w, down_w)
    slot_out = jnp.where(
        live_row[:, None],
        merged[jnp.where(live_row, position, 0)],
        jnp.zeros((total_rows, width), jnp.bfloat16),
    )
    summed = lax.psum_scatter(
        slot_out.reshape(n_dp * n_exp, slot_cap, width), "dp", scatter_dimension=0, tiled=True
    ).astype(jnp.float32)
    expert_out = lax.all_to_all(
        summed.astype(jnp.bfloat16), "expert", split_axis=0, concat_axis=0, tiled=True
    )
    picked = expert_out.reshape(n_exp * slot_cap, width)[slot_idx]
    gate_wts = jnp.exp(gate_logits)
    gate_wts = gate_wts / jnp.sum(gate_wts, axis=1, keepdims=True)
    mixed = jnp.sum(
        picked.reshape(n_rows, n_tops, width).astype(jnp.float32) * gate_wts[:, :, None], axis=1
    )
    return mixed.astype(jnp.bfloat16)


LANES = 128
CHUNKS = 1


def round_up(value, step):
    return (value + step - 1) // step * step


def routing_columns(expert_ids, gate_logits, n_exp, lanes):
    gate_wts = jnp.exp(gate_logits)
    gate_wts = gate_wts / jnp.sum(gate_wts, axis=1, keepdims=True)
    chosen = expert_ids[:, :, None] == jnp.arange(n_exp, dtype=jnp.int32)[None, None, :]
    by_expert = jnp.sum(jnp.where(chosen, gate_wts[:, :, None], 0.0), axis=1)
    high = by_expert.astype(jnp.bfloat16)
    low = (by_expert - high.astype(jnp.float32)).astype(jnp.bfloat16)
    columns = jnp.concatenate([high, low], axis=1)
    return jnp.pad(columns, ((0, 0), (0, lanes - columns.shape[1])))


def dense_kernel(n_exp, rows_ref, gate_ref, up_ref, down_ref, out_ref):
    width, hidden_width = gate_ref.shape
    lanes = rows_ref.shape[1]
    mine = lax.axis_index("expert")
    rows_in = rows_ref[:, :width]
    gate_val = jnp.dot(rows_in, gate_ref[...], preferred_element_type=jnp.float32)
    up_val = jnp.dot(rows_in, up_ref[...], preferred_element_type=jnp.float32)
    first = width // LANES * LANES
    extra = rows_ref[:, first:lanes].astype(jnp.float32)
    lane = lax.broadcasted_iota(jnp.int32, extra.shape, 1) + first - width
    weight = jnp.sum(jnp.where((lane == mine) | (lane == mine + n_exp), extra, 0.0), axis=1, keepdims=True)
    hidden = (up_val + 1.0) * gate_val * (weight / (1.0 + jnp.exp(-1.702 * gate_val)))
    out_ref[...] = jnp.dot(
        hidden.astype(jnp.bfloat16), down_ref[...], preferred_element_type=jnp.float32
    ).astype(out_ref.dtype)


def dense_rows(rows, gate_w, up_w, down_w, n_exp):
    n_rows, lanes = rows.shape
    width, hidden_width = gate_w.shape
    tile_rows = 256
    while n_rows % tile_rows:
        tile_rows //= 2
    whole = pl.BlockSpec(memory_space=pltpu.VMEM)
    return pl.pallas_call(
        functools.partial(dense_kernel, n_exp),
        grid=(n_rows // tile_rows,),
        in_specs=[pl.BlockSpec((tile_rows, lanes), lambda i: (i, 0)), whole, whole, whole],
        out_specs=pl.BlockSpec((tile_rows, width), lambda i: (i, 0)),
        out_shape=jax.ShapeDtypeStruct((n_rows, width), jnp.bfloat16),
        cost_estimate=pl.CostEstimate(
            flops=6 * n_rows * width * hidden_width,
            bytes_accessed=2 * n_rows * (lanes + width) + 6 * width * hidden_width,
            transcendentals=n_rows * hidden_width,
        ),
    )(rows, gate_w, up_w, down_w)


def dense_device(tokens, expert_ids, gate_logits, w_gate, w_up, w_down):
    n_rows, width = tokens.shape
    n_exp = lax.axis_size("expert")
    both = ("expert", "dp")
    lanes = round_up(width + 2 * n_exp, LANES)
    extra = routing_columns(expert_ids, gate_logits, n_exp, lanes - width)
    wide = jnp.concatenate([tokens, extra], axis=1)
    step = n_rows // CHUNKS
    done = []
    for chunk in range(CHUNKS):
        rows = lax.all_gather(wide[chunk * step : (chunk + 1) * step], both, axis=0, tiled=True)
        partial = dense_rows(rows, w_gate[0], w_up[0], w_down[0], n_exp)
        done.append(lax.psum_scatter(partial, both, scatter_dimension=0, tiled=True))
    return done[0] if CHUNKS == 1 else jnp.concatenate(done, axis=0)


def tile_product(n_exp, rows_in, extra, gate_ref, up_ref, down_ref):
    width = gate_ref.shape[0]
    mine = lax.axis_index("expert")
    gate_val = jnp.dot(rows_in, gate_ref[...], preferred_element_type=jnp.float32)
    up_val = jnp.dot(rows_in, up_ref[...], preferred_element_type=jnp.float32)
    extra = extra.astype(jnp.float32)
    lane = lax.broadcasted_iota(jnp.int32, extra.shape, 1) - width % LANES
    weight = jnp.sum(jnp.where((lane == mine) | (lane == mine + n_exp), extra, 0.0), axis=1, keepdims=True)
    hidden = (up_val + 1.0) * gate_val * (weight / (1.0 + jnp.exp(-1.702 * gate_val)))
    return jnp.dot(hidden.astype(jnp.bfloat16), down_ref[...], preferred_element_type=jnp.float32)


def fused_kernel(
    n_exp, wide_ref, gate_hbm, up_hbm, down_hbm, out_ref,
    held, part, core_in, x_in, y_in, x_diag, y_diag, z_in,
    gate_ref, up_ref, down_ref, send_sem, recv_sem, load_sem,
):
    n_z = n_exp // 2
    n_rows, width = out_ref.shape
    lanes = wide_ref.shape[1]
    half = n_rows // 2
    spare = width // LANES * LANES
    expert, dp = lax.axis_index("expert"), lax.axis_index("dp")
    z, y = lax.div(expert, 2), lax.rem(expert, 2)
    x, core = lax.div(dp, 2), lax.rem(dp, 2)
    to_x = (expert, (1 - x) * 2 + core)
    to_y = (z * 2 + 1 - y, dp)
    to_core = (expert, x * 2 + 1 - core)

    def at_z(d):
        return lax.rem(z + d, n_z)

    def to_z(d):
        return (at_z(d) * 2 + y, dp)

    columns = {"o": y * 2 + x, "x": y * 2 + 1 - x, "y": (1 - y) * 2 + x, "d": (1 - y) * 2 + 1 - x}

    def block(column, which, zz=0):
        return (columns[column] * 2 + which) * n_z + zz

    copies = {}

    def start(key, source, target, device):
        number = len(copies)
        copies[key] = pltpu.make_async_remote_copy(
            src_ref=source,
            dst_ref=target,
            send_sem=send_sem.at[number],
            recv_sem=recv_sem.at[number],
            device_id=device,
            device_id_type=pl.DeviceIdType.MESH,
        )
        copies[key].start()

    def arrived(*key):
        copies[key].wait_recv()

    loads = [
        pltpu.make_async_copy(source, target, load_sem.at[i])
        for i, (source, target) in enumerate(((gate_hbm, gate_ref), (up_hbm, up_ref), (down_hbm, down_ref)))
    ]
    for load in loads:
        load.start()

    partners = [to_x, to_y, to_core] + [to_z(d) for d in range(1, n_z)]
    barrier = pltpu.get_barrier_semaphore()
    for partner in partners:
        pl.semaphore_signal(barrier, inc=1, device_id=partner, device_id_type=pl.DeviceIdType.MESH)
    pl.semaphore_wait(barrier, len(partners))

    near = sorted(range(1, n_z), key=lambda d: min(d, n_z - d))
    own = held.at[block("o", core, z)]
    start(("x", 0), wide_ref, own, to_x)
    start(("y", 0), wide_ref, own, to_y)
    for d in near:
        start(("z", d), wide_ref, own, to_z(d))
    start(("co", 0), wide_ref, own, to_core)
    own[...] = wide_ref[...]

    def relay_z(d):
        arrived("z", d)
        source = held.at[block("o", core, at_z(n_z - d))]
        start(("x", d), source, source, to_x)
        start(("y", d), source, source, to_y)
        start(("co", d), source, source, to_core)

    def relay_xy(d):
        zz = at_z(n_z - d)
        arrived("x", d)
        source = held.at[block("x", core, zz)]
        upper = held.at[block("x", core, zz), pl.ds(0, half)]
        start(("y2", d), upper, upper, to_y)
        start(("cx", d), source, source, to_core)
        arrived("y", d)
        source = held.at[block("y", core, zz)]
        lower = held.at[block("y", core, zz), pl.ds(half, half)]
        start(("x2", d), lower, lower, to_x)
        start(("cy", d), source, source, to_core)

    def relay_diag(d):
        source = held.at[block("d", core, at_z(n_z - d))]
        arrived("x2", d)
        arrived("y2", d)
        start(("cd", d), source, source, to_core)

    def product(column, which):
        span = pl.ds(block(column, which), n_z)
        rows_in = held[span, :, :width].reshape(n_z * n_rows, width)
        extra = held[span, :, spare:lanes].reshape(n_z * n_rows, lanes - spare)
        result = tile_product(n_exp, rows_in, extra, gate_ref, up_ref, down_ref)
        part[span] = result.astype(part.dtype).reshape(n_z, n_rows, width)

    order = "oxyd"

    def swap(column):
        for d in range(n_z):
            arrived("c" + column, d)
        product(column, 1 - core)
        start(("p", column), part.at[pl.ds(block(column, 1 - core), n_z)], core_in.at[order.index(column)], to_core)

    def combine(column):
        arrived("p", column)
        place = order.index(column)
        base = block(column, core)

        @pl.loop(0, n_z)
        def _(zz):
            part[base + zz] = part[base + zz] + core_in[place, zz]

    waiting = [0]
    for d in near:
        relay_z(d)
        if d == near[-1]:
            for load in loads:
                load.wait()
            product("o", core)
        relay_xy(waiting.pop())
        waiting.append(d)
    swap("o")
    relay_xy(waiting.pop())
    product("x", core)
    swap("x")
    relay_diag(0)
    product("y", core)
    for d in near[:-1]:
        relay_diag(d)
    swap("y")
    relay_diag(near[-1])
    combine("x")
    rows_x = pl.ds(block("x", core), n_z)
    start(("ex",), part.at[rows_x, pl.ds(half, half)], x_in.at[:, pl.ds(half, half)], to_x)
    combine("y")
    rows_y = pl.ds(block("y", core), n_z)
    start(("ey",), part.at[rows_y, pl.ds(0, half)], y_in.at[:, pl.ds(0, half)], to_y)
    product("d", core)
    swap("d")
    combine("d")
    far = near[::-1] + [0]
    for d in far:
        source = block("d", core, at_z(d))
        start(("dx", d), part.at[source, pl.ds(half, half)], x_diag.at[d], to_x)
        start(("dy", d), part.at[source, pl.ds(0, half)], y_diag.at[d], to_y)
    combine("o")

    def gather_diag(d):
        zz = at_z(d)
        arrived("dx", d)
        spot = block("y", core, zz)
        part[spot, half:] = part[spot, half:] + x_diag[d]
        start(("fy", d), part.at[spot, pl.ds(half, half)], y_in.at[zz, pl.ds(half, half)], to_y)
        arrived("dy", d)
        spot = block("x", core, zz)
        part[spot, :half] = part[spot, :half] + y_diag[d]
        start(("fx", d), part.at[spot, pl.ds(0, half)], x_in.at[zz, pl.ds(0, half)], to_x)

    def gather_xy(d):
        zz = at_z(d)
        arrived("fx", d)
        arrived("fy", d)
        total = (
            part[block("o", core, zz)].astype(jnp.float32)
            + x_in[zz].astype(jnp.float32)
            + y_in[zz].astype(jnp.float32)
        )
        if d == 0:
            for other in far[:-1]:
                arrived("s", other)
                total = total + z_in[other - 1].astype(jnp.float32)
            out_ref[...] = total.astype(out_ref.dtype)
        else:
            spot = block("o", core, zz)
            part[spot] = total.astype(part.dtype)
            start(("s", d), part.at[spot], z_in.at[d - 1], to_z(d))

    gather_diag(far[0])
    arrived("ex")
    arrived("ey")
    for before, d in zip(far, far[1:]):
        gather_diag(d)
        gather_xy(before)
    gather_xy(far[-1])
    for copy in copies.values():
        copy.wait_send()


def fused_device(tokens, expert_ids, gate_logits, w_gate, w_up, w_down):
    n_rows, width = tokens.shape
    hidden_width = w_gate.shape[2]
    n_exp = lax.axis_size("expert")
    n_z = n_exp // 2
    lanes = round_up(width + 2 * n_exp, LANES)
    extra = routing_columns(expert_ids, gate_logits, n_exp, lanes - width)
    wide = jnp.concatenate([tokens, extra], axis=1)
    total = n_exp * lax.axis_size("dp")
    messages = 8 * n_z + 4 * n_z + 4 + 2 + 4 * n_z + n_z + n_z
    bf16 = jnp.bfloat16
    in_vmem = pl.BlockSpec(memory_space=pltpu.VMEM)
    anywhere = pl.BlockSpec(memory_space=pl.ANY)
    return pl.pallas_call(
        functools.partial(fused_kernel, n_exp),
        in_specs=[in_vmem, anywhere, anywhere, anywhere],
        out_specs=in_vmem,
        out_shape=jax.ShapeDtypeStruct((n_rows, width), bf16),
        scratch_shapes=[
            pltpu.VMEM((total, n_rows, lanes), bf16),
            pltpu.VMEM((total, n_rows, width), bf16),
            pltpu.VMEM((4, n_z, n_rows, width), bf16),
            pltpu.VMEM((n_z, n_rows, width), bf16),
            pltpu.VMEM((n_z, n_rows, width), bf16),
            pltpu.VMEM((n_z, n_rows // 2, width), bf16),
            pltpu.VMEM((n_z, n_rows // 2, width), bf16),
            pltpu.VMEM((n_z - 1, n_rows, width), bf16),
            pltpu.VMEM((width, hidden_width), bf16),
            pltpu.VMEM((width, hidden_width), bf16),
            pltpu.VMEM((hidden_width, width), bf16),
            pltpu.SemaphoreType.DMA((messages,)),
            pltpu.SemaphoreType.DMA((messages,)),
            pltpu.SemaphoreType.DMA((3,)),
        ],
        compiler_params=pltpu.CompilerParams(
            collective_id=0, has_side_effects=True, vmem_limit_bytes=64 * 1024 * 1024 - 65536
        ),
    )(wide, w_gate[0], w_up[0], w_down[0])


def solution(mesh):
    def per_device(tokens, expert_ids, *others):
        n_exp = lax.axis_size("expert")
        if n_exp > 4 * expert_ids.shape[1]:
            return sparse_device(tokens, expert_ids, *others)
        paired = lax.axis_size("dp") == 4 and n_exp % 2 == 0 and tokens.shape[0] % 32 == 0
        return (fused_device if paired else dense_device)(tokens, expert_ids, *others)

    return jax.shard_map(
        per_device,
        mesh=mesh,
        in_specs=(
            P(("expert", "dp"), None),
            P(("expert", "dp"), None),
            P(("expert", "dp"), None),
            P("expert", None, "dp"),
            P("expert", None, "dp"),
            P("expert", "dp", None),
        ),
        out_specs=P(("expert", "dp"), None),
        check_vma=False,
    )
```

```python
import functools

import jax
import jax.numpy as jnp
from jax import lax
from jax.experimental import pallas as pl
from jax.experimental.pallas import tpu as pltpu
from jax.sharding import PartitionSpec as P


def expert_rows(tile_in, gate_w, up_w, down_w):
    gate_val = jnp.dot(tile_in, gate_w, preferred_element_type=jnp.float32)
    up_val = jnp.dot(tile_in, up_w, preferred_element_type=jnp.float32)
    hidden = ((up_val + 1.0) * gate_val * jax.nn.sigmoid(1.702 * gate_val)).astype(jnp.bfloat16)
    return jnp.dot(hidden, down_w, preferred_element_type=jnp.float32).astype(jnp.bfloat16)


def run_tiles(packed, first_row, last_row, gate_w, up_w, down_w):
    tile_rows = 128
    n_tiles = jnp.maximum(last_row - first_row + tile_rows - 1, 0) // tile_rows
    result_buf = jnp.zeros((packed.shape[0], down_w.shape[1]), jnp.bfloat16)

    def advance(index_t, buffer):
        at_row = first_row + index_t * tile_rows
        tile_in = lax.dynamic_slice_in_dim(packed, at_row, tile_rows, 0)
        return lax.dynamic_update_slice_in_dim(
            buffer, expert_rows(tile_in, gate_w, up_w, down_w), at_row, 0
        )

    return lax.fori_loop(0, n_tiles, advance, result_buf)


def sparse_device(tokens, expert_ids, gate_logits, w_gate, w_up, w_down):
    n_rows, width = tokens.shape
    n_tops = expert_ids.shape[1]
    n_exp = lax.axis_size("expert")
    n_dp = lax.axis_size("dp")
    slot_cap = max(2, 3 * n_rows * n_tops // (2 * n_exp))
    tile_rows = 128
    flat_ids = expert_ids.reshape(-1)
    onehot = (flat_ids[:, None] == jnp.arange(n_exp, dtype=jnp.int32)[None, :]).astype(jnp.int32)
    rank_in = jnp.sum((jnp.cumsum(onehot, axis=0) - onehot) * onehot, axis=1)
    counts = jnp.sum(onehot, axis=0)
    slot_idx = flat_ids * slot_cap + rank_in
    source = (
        jnp.zeros((n_exp * slot_cap,), jnp.int32)
        .at[slot_idx]
        .set(jnp.arange(n_rows * n_tops, dtype=jnp.int32) // n_tops)
    )
    filled = (jnp.arange(slot_cap)[None, :] < counts[:, None]).reshape(-1)
    outgoing = jnp.where(filled[:, None], tokens[source], jnp.zeros_like(tokens[source])).reshape(
        n_exp, slot_cap, width
    )
    rows_mid, counts_mid = (
        lax.all_to_all(outgoing, "expert", split_axis=0, concat_axis=0, tiled=True),
        lax.all_to_all(counts[:, None], "expert", split_axis=0, concat_axis=0, tiled=True),
    )
    rows_in, counts_in = (
        lax.all_gather(rows_mid, "dp", axis=0, tiled=True),
        lax.all_gather(counts_mid, "dp", axis=0, tiled=True),
    )
    rows_flat = rows_in.reshape(-1, width)
    total_rows = rows_flat.shape[0]
    live_row = (jnp.arange(slot_cap)[None, :] < counts_in.reshape(-1)[:, None]).reshape(-1)
    position = jnp.cumsum(live_row.astype(jnp.int32)) - 1
    live_total = jnp.sum(live_row.astype(jnp.int32))
    padded = (total_rows + tile_rows - 1) // tile_rows * tile_rows + tile_rows
    gather_idx = (
        jnp.zeros((padded,), jnp.int32)
        .at[jnp.where(live_row, position, padded)]
        .set(jnp.arange(total_rows, dtype=jnp.int32), mode="drop")
    )
    packed = rows_flat[gather_idx]
    gate_w = w_gate[0]
    up_w = w_up[0]
    down_w = w_down[0]
    merged = run_tiles(packed, 0, live_total, gate_w, up_w, down_w)
    slot_out = jnp.where(
        live_row[:, None],
        merged[jnp.where(live_row, position, 0)],
        jnp.zeros((total_rows, width), jnp.bfloat16),
    )
    summed = lax.psum_scatter(
        slot_out.reshape(n_dp * n_exp, slot_cap, width), "dp", scatter_dimension=0, tiled=True
    ).astype(jnp.float32)
    expert_out = lax.all_to_all(
        summed.astype(jnp.bfloat16), "expert", split_axis=0, concat_axis=0, tiled=True
    )
    picked = expert_out.reshape(n_exp * slot_cap, width)[slot_idx]
    gate_wts = jnp.exp(gate_logits)
    gate_wts = gate_wts / jnp.sum(gate_wts, axis=1, keepdims=True)
    mixed = jnp.sum(
        picked.reshape(n_rows, n_tops, width).astype(jnp.float32) * gate_wts[:, :, None], axis=1
    )
    return mixed.astype(jnp.bfloat16)


LANES = 128
CHUNKS = 1


def round_up(value, step):
    return (value + step - 1) // step * step


def routing_columns(expert_ids, gate_logits, n_exp, lanes):
    gate_wts = jnp.exp(gate_logits)
    gate_wts = gate_wts / jnp.sum(gate_wts, axis=1, keepdims=True)
    chosen = expert_ids[:, :, None] == jnp.arange(n_exp, dtype=jnp.int32)[None, None, :]
    by_expert = jnp.sum(jnp.where(chosen, gate_wts[:, :, None], 0.0), axis=1)
    high = by_expert.astype(jnp.bfloat16)
    low = (by_expert - high.astype(jnp.float32)).astype(jnp.bfloat16)
    columns = jnp.concatenate([high, low], axis=1)
    return jnp.pad(columns, ((0, 0), (0, lanes - columns.shape[1])))


def dense_kernel(n_exp, rows_ref, gate_ref, up_ref, down_ref, out_ref):
    width, hidden_width = gate_ref.shape
    lanes = rows_ref.shape[1]
    mine = lax.axis_index("expert")
    rows_in = rows_ref[:, :width]
    gate_val = jnp.dot(rows_in, gate_ref[...], preferred_element_type=jnp.float32)
    up_val = jnp.dot(rows_in, up_ref[...], preferred_element_type=jnp.float32)
    first = width // LANES * LANES
    extra = rows_ref[:, first:lanes].astype(jnp.float32)
    lane = lax.broadcasted_iota(jnp.int32, extra.shape, 1) + first - width
    weight = jnp.sum(jnp.where((lane == mine) | (lane == mine + n_exp), extra, 0.0), axis=1, keepdims=True)
    hidden = (up_val + 1.0) * gate_val * (weight / (1.0 + jnp.exp(-1.702 * gate_val)))
    out_ref[...] = jnp.dot(
        hidden.astype(jnp.bfloat16), down_ref[...], preferred_element_type=jnp.float32
    ).astype(out_ref.dtype)


def dense_rows(rows, gate_w, up_w, down_w, n_exp):
    n_rows, lanes = rows.shape
    width, hidden_width = gate_w.shape
    tile_rows = 256
    while n_rows % tile_rows:
        tile_rows //= 2
    whole = pl.BlockSpec(memory_space=pltpu.VMEM)
    return pl.pallas_call(
        functools.partial(dense_kernel, n_exp),
        grid=(n_rows // tile_rows,),
        in_specs=[pl.BlockSpec((tile_rows, lanes), lambda i: (i, 0)), whole, whole, whole],
        out_specs=pl.BlockSpec((tile_rows, width), lambda i: (i, 0)),
        out_shape=jax.ShapeDtypeStruct((n_rows, width), jnp.bfloat16),
        cost_estimate=pl.CostEstimate(
            flops=6 * n_rows * width * hidden_width,
            bytes_accessed=2 * n_rows * (lanes + width) + 6 * width * hidden_width,
            transcendentals=n_rows * hidden_width,
        ),
    )(rows, gate_w, up_w, down_w)


def dense_device(tokens, expert_ids, gate_logits, w_gate, w_up, w_down):
    n_rows, width = tokens.shape
    n_exp = lax.axis_size("expert")
    both = ("expert", "dp")
    lanes = round_up(width + 2 * n_exp, LANES)
    extra = routing_columns(expert_ids, gate_logits, n_exp, lanes - width)
    wide = jnp.concatenate([tokens, extra], axis=1)
    step = n_rows // CHUNKS
    done = []
    for chunk in range(CHUNKS):
        rows = lax.all_gather(wide[chunk * step : (chunk + 1) * step], both, axis=0, tiled=True)
        partial = dense_rows(rows, w_gate[0], w_up[0], w_down[0], n_exp)
        done.append(lax.psum_scatter(partial, both, scatter_dimension=0, tiled=True))
    return done[0] if CHUNKS == 1 else jnp.concatenate(done, axis=0)


def tile_product(n_exp, rows_in, extra, gate_ref, up_ref, down_ref):
    width = gate_ref.shape[0]
    mine = lax.axis_index("expert")
    gate_val = jnp.dot(rows_in, gate_ref[...], preferred_element_type=jnp.float32)
    up_val = jnp.dot(rows_in, up_ref[...], preferred_element_type=jnp.float32)
    extra = extra.astype(jnp.float32)
    lane = lax.broadcasted_iota(jnp.int32, extra.shape, 1) - width % LANES
    weight = jnp.sum(jnp.where((lane == mine) | (lane == mine + n_exp), extra, 0.0), axis=1, keepdims=True)
    hidden = (up_val + 1.0) * gate_val * (weight / (1.0 + jnp.exp(-1.702 * gate_val)))
    return lax.dot_general(
        hidden.astype(jnp.bfloat16),
        down_ref[...],
        (((1,), (1,)), ((), ())),
        preferred_element_type=jnp.float32,
    )


def fused_kernel(
    n_exp, wide_ref, gate_hbm, up_hbm, down_hbm, out_ref,
    held, part, core_in, x_in, y_in, x_diag, y_diag, z_in,
    gate_ref, up_ref, down_ref, send_sem, recv_sem, load_sem,
):
    n_z = n_exp // 2
    n_rows, width = out_ref.shape
    lanes = wide_ref.shape[1]
    half = n_rows // 2
    spare = width // LANES * LANES
    expert, dp = lax.axis_index("expert"), lax.axis_index("dp")
    z, y = lax.div(expert, 2), lax.rem(expert, 2)
    x, core = lax.div(dp, 2), lax.rem(dp, 2)
    to_x = (expert, (1 - x) * 2 + core)
    to_y = (z * 2 + 1 - y, dp)
    to_core = (expert, x * 2 + 1 - core)

    def at_z(d):
        return lax.rem(z + d, n_z)

    def to_z(d):
        return (at_z(d) * 2 + y, dp)

    columns = {"o": y * 2 + x, "x": y * 2 + 1 - x, "y": (1 - y) * 2 + x, "d": (1 - y) * 2 + 1 - x}

    def block(column, which, zz=0):
        return (columns[column] * 2 + which) * n_z + zz

    copies = {}

    def start(key, source, target, device):
        number = len(copies)
        copies[key] = pltpu.make_async_remote_copy(
            src_ref=source,
            dst_ref=target,
            send_sem=send_sem.at[number],
            recv_sem=recv_sem.at[number],
            device_id=device,
            device_id_type=pl.DeviceIdType.MESH,
        )
        copies[key].start()

    def arrived(*key):
        copies[key].wait_recv()

    loads = [
        pltpu.make_async_copy(source, target, load_sem.at[i])
        for i, (source, target) in enumerate(((gate_hbm, gate_ref), (up_hbm, up_ref), (down_hbm, down_ref)))
    ]
    for load in loads:
        load.start()

    partners = [to_x, to_y, to_core] + [to_z(d) for d in range(1, n_z)]
    barrier = pltpu.get_barrier_semaphore()
    for partner in partners:
        pl.semaphore_signal(barrier, inc=1, device_id=partner, device_id_type=pl.DeviceIdType.MESH)
    pl.semaphore_wait(barrier, len(partners))

    near = sorted(range(1, n_z), key=lambda d: min(d, n_z - d))
    own = held.at[block("o", core, z)]
    start(("x", 0), wide_ref, own, to_x)
    start(("y", 0), wide_ref, own, to_y)
    for d in near:
        start(("z", d), wide_ref, own, to_z(d))
    start(("co", 0), wide_ref, own, to_core)
    own[...] = wide_ref[...]

    def relay_z(d):
        arrived("z", d)
        source = held.at[block("o", core, at_z(n_z - d))]
        start(("x", d), source, source, to_x)
        start(("y", d), source, source, to_y)
        start(("co", d), source, source, to_core)

    def relay_xy(d):
        zz = at_z(n_z - d)
        arrived("x", d)
        source = held.at[block("x", core, zz)]
        upper = held.at[block("x", core, zz), pl.ds(0, half)]
        start(("y2", d), upper, upper, to_y)
        start(("cx", d), source, source, to_core)
        arrived("y", d)
        source = held.at[block("y", core, zz)]
        lower = held.at[block("y", core, zz), pl.ds(half, half)]
        start(("x2", d), lower, lower, to_x)
        start(("cy", d), source, source, to_core)

    def relay_diag(d):
        source = held.at[block("d", core, at_z(n_z - d))]
        arrived("x2", d)
        arrived("y2", d)
        start(("cd", d), source, source, to_core)

    def product(column, which):
        span = pl.ds(block(column, which), n_z)
        rows_in = held[span, :, :width].reshape(n_z * n_rows, width)
        extra = held[span, :, spare:lanes].reshape(n_z * n_rows, lanes - spare)
        result = tile_product(n_exp, rows_in, extra, gate_ref, up_ref, down_ref)
        part[span] = result.astype(part.dtype).reshape(n_z, n_rows, width)

    order = "oxyd"

    def swap(column):
        for d in range(n_z):
            arrived("c" + column, d)
        product(column, 1 - core)
        start(("p", column), part.at[pl.ds(block(column, 1 - core), n_z)], core_in.at[order.index(column)], to_core)

    def combine(column):
        arrived("p", column)
        place = order.index(column)
        base = block(column, core)

        @pl.loop(0, n_z)
        def _(zz):
            part[base + zz] = part[base + zz] + core_in[place, zz]

    waiting = [0]
    for d in near:
        relay_z(d)
        if d == near[-1]:
            for load in loads:
                load.wait()
            product("o", core)
        relay_xy(waiting.pop())
        waiting.append(d)
    swap("o")
    relay_xy(waiting.pop())
    product("x", core)
    swap("x")
    relay_diag(0)
    product("y", core)
    for d in near[:-1]:
        relay_diag(d)
    combine("x")
    rows_x = pl.ds(block("x", core), n_z)
    start(("ex",), part.at[rows_x, pl.ds(half, half)], x_in.at[:, pl.ds(half, half)], to_x)
    swap("y")
    relay_diag(near[-1])
    product("d", core)
    combine("y")
    rows_y = pl.ds(block("y", core), n_z)
    start(("ey",), part.at[rows_y, pl.ds(0, half)], y_in.at[:, pl.ds(0, half)], to_y)
    swap("d")
    combine("d")
    far = near[::-1] + [0]
    for d in far:
        source = block("d", core, at_z(d))
        start(("dx", d), part.at[source, pl.ds(half, half)], x_diag.at[d], to_x)
        start(("dy", d), part.at[source, pl.ds(0, half)], y_diag.at[d], to_y)
    combine("o")

    def gather_diag(d):
        zz = at_z(d)
        arrived("dx", d)
        spot = block("y", core, zz)
        part[spot, half:] = part[spot, half:] + x_diag[d]
        start(("fy", d), part.at[spot, pl.ds(half, half)], y_in.at[zz, pl.ds(half, half)], to_y)
        arrived("dy", d)
        spot = block("x", core, zz)
        part[spot, :half] = part[spot, :half] + y_diag[d]
        start(("fx", d), part.at[spot, pl.ds(0, half)], x_in.at[zz, pl.ds(0, half)], to_x)

    def gather_xy(d):
        zz = at_z(d)
        arrived("fx", d)
        arrived("fy", d)
        total = (
            part[block("o", core, zz)].astype(jnp.float32)
            + x_in[zz].astype(jnp.float32)
            + y_in[zz].astype(jnp.float32)
        )
        if d == 0:
            for other in far[:-1]:
                arrived("s", other)
                total = total + z_in[other - 1].astype(jnp.float32)
            out_ref[...] = total.astype(out_ref.dtype)
        else:
            spot = block("o", core, zz)
            part[spot] = total.astype(part.dtype)
            start(("s", d), part.at[spot], z_in.at[d - 1], to_z(d))

    gather_diag(far[0])
    arrived("ex")
    arrived("ey")
    for before, d in zip(far, far[1:]):
        gather_diag(d)
        gather_xy(before)
    gather_xy(far[-1])
    for copy in copies.values():
        copy.wait_send()


def fused_device(tokens, expert_ids, gate_logits, w_gate, w_up, w_down):
    n_rows, width = tokens.shape
    hidden_width = w_gate.shape[2]
    n_exp = lax.axis_size("expert")
    n_z = n_exp // 2
    lanes = round_up(width + 2 * n_exp, LANES)
    extra = routing_columns(expert_ids, gate_logits, n_exp, lanes - width)
    wide = jnp.concatenate([tokens, extra], axis=1)
    total = n_exp * lax.axis_size("dp")
    messages = 8 * n_z + 4 * n_z + 4 + 2 + 4 * n_z + n_z + n_z
    bf16 = jnp.bfloat16
    in_vmem = pl.BlockSpec(memory_space=pltpu.VMEM)
    anywhere = pl.BlockSpec(memory_space=pl.ANY)
    return pl.pallas_call(
        functools.partial(fused_kernel, n_exp),
        in_specs=[in_vmem, anywhere, anywhere, anywhere],
        out_specs=in_vmem,
        out_shape=jax.ShapeDtypeStruct((n_rows, width), bf16),
        scratch_shapes=[
            pltpu.VMEM((total, n_rows, lanes), bf16),
            pltpu.VMEM((total, n_rows, width), bf16),
            pltpu.VMEM((4, n_z, n_rows, width), bf16),
            pltpu.VMEM((n_z, n_rows, width), bf16),
            pltpu.VMEM((n_z, n_rows, width), bf16),
            pltpu.VMEM((n_z, n_rows // 2, width), bf16),
            pltpu.VMEM((n_z, n_rows // 2, width), bf16),
            pltpu.VMEM((n_z - 1, n_rows, width), bf16),
            pltpu.VMEM((width, hidden_width), bf16),
            pltpu.VMEM((width, hidden_width), bf16),
            pltpu.VMEM((width, hidden_width), bf16),
            pltpu.SemaphoreType.DMA((messages,)),
            pltpu.SemaphoreType.DMA((messages,)),
            pltpu.SemaphoreType.DMA((3,)),
        ],
        compiler_params=pltpu.CompilerParams(
            collective_id=0, has_side_effects=True, vmem_limit_bytes=64 * 1024 * 1024 - 65536
        ),
    )(wide, w_gate[0], w_up[0], w_down[0].T)


def solution(mesh):
    def per_device(tokens, expert_ids, *others):
        n_exp = lax.axis_size("expert")
        if n_exp > 4 * expert_ids.shape[1]:
            return sparse_device(tokens, expert_ids, *others)
        paired = lax.axis_size("dp") == 4 and n_exp % 2 == 0 and tokens.shape[0] % 32 == 0
        return (fused_device if paired else dense_device)(tokens, expert_ids, *others)

    return jax.shard_map(
        per_device,
        mesh=mesh,
        in_specs=(
            P(("expert", "dp"), None),
            P(("expert", "dp"), None),
            P(("expert", "dp"), None),
            P("expert", None, "dp"),
            P("expert", None, "dp"),
            P("expert", "dp", None),
        ),
        out_specs=P(("expert", "dp"), None),
        check_vma=False,
    )
```
